32 devices in a mesh: lat: 8 (over z, y), lev: 4 (over x, core).
Axes of the slice: x: 2, y: 2, z: 4, core: 2. Of those that a mesh axis runs over, the one named last changes fastest.
Arguments:
- assign: int32 [640], replicated, may hold values from 0 to 639, each once
- u_spec: bfloat16 [640, 32, 2, 640], P('lat', 'lev'), may hold values from -0.25 to 0.25
- v_spec: bfloat16 [640, 32, 2, 640], P('lat', 'lev'), may hold values from -0.25 to 0.25
- basis: bfloat16 [640, 640, 640], P('lat', 'lev'), may hold values from -0.25 to 0.25
Outputs:
- vort_spec: float32 [640, 32, 2, 640], P('lat', 'lev')
The draws below stay inside these ranges and needn't reach their ends.
Inputs may be any that keep to these rules, and one draw needn't show every extreme that they name: Row k of u_spec, v_spec, basis and vort_spec belongs to zonal wavenumber assign[k]; each of the 640 wavenumbers appears once.
All inputs are finite; a program needn't handle non-finite values.
Results may differ from the reference program's by a relative error of at most 0.0061.
Values may be sent and summed in bfloat16 or wider, within the bound.
A program may use at most 256 MiB of HBM per device.

```python
import math
import jax
import jax.numpy as jnp
from jax import lax

M = 640
LAT = 1280
LON = 2560
LEVELS = 32
HALF = 640


def block_levels(stream_key, extent, shards, smallest, high):
    def one(position, blocks):
        steps = jax.random.uniform(jax.random.fold_in(jax.random.fold_in(stream_key, 6), position), (blocks,), jnp.float32, smallest / len(shards), high / len(shards))
        return jnp.repeat(jnp.exp(steps), extent[position] // blocks).reshape((-1,) + (1,) * (len(extent) - position - 1))

    factor_of = one(*shards[0])
    for cut in shards[1:]:
        factor_of = factor_of * one(*cut)
    return factor_of


def gaussian(key, extent, scale, bound, split=(), kind=jnp.bfloat16):
    drawn = scale * jax.random.normal(key, extent, jnp.float32)
    if split:
        drawn = drawn * block_levels(key, extent, split, -0.22, 0.18)
    return jnp.clip(drawn, -bound, bound).astype(kind)


def setup_inputs(seed: int = 0) -> dict:
    splits = jax.random.split(jax.random.key(seed), 5)
    assign = jax.random.permutation(splits[0], M).astype(jnp.int32)
    u_spec = gaussian(splits[1], (M, LEVELS, 2, M), M ** -0.5, 0.25, ((0, 8), (1, 4)))
    v_spec = gaussian(splits[2], (M, LEVELS, 2, M), M ** -0.5, 0.25, ((0, 8), (1, 4)))
    basis = gaussian(splits[3], (M, HALF, M), M ** -0.5, 0.25, ((0, 8), (1, 4)))
    return {"assign": assign, "u_spec": u_spec, "v_spec": v_spec, "basis": basis}


def degree_factors(wavenums):
    degree = jnp.arange(M, dtype=jnp.int32)
    live_mask = (degree[None, :] >= wavenums[:, None]).astype(jnp.int32)
    parity = 1 - 2 * ((degree[None, :] + wavenums[:, None]) % 2)
    return (live_mask, live_mask * parity)

def zonal_tables(wavenums):
    columns = jnp.arange(LON, dtype=jnp.int32)
    phases = wavenums[:, None] * columns[None, :] % LON
    angles = phases.astype(jnp.float32) * (2.0 * math.pi / LON)
    return jnp.stack([jnp.cos(angles), jnp.sin(angles)], axis=0).astype(jnp.bfloat16)

def reference(assign, u_spec, v_spec, basis):
    assign = assign.astype(jnp.int32)
    half_rows = LAT // 2
    live_mask, signed = degree_factors(assign)
    spectra = jnp.stack([u_spec, v_spec], axis=2).reshape(M, LEVELS * 4, M)

    def meridional(inputs):
        coeffs, live_row, signed_row, legendre = inputs
        masked = coeffs * live_row.astype(jnp.bfloat16)[None, :]
        flipped = coeffs * signed_row.astype(jnp.bfloat16)[None, :]
        northern = jnp.dot(legendre, masked.T, preferred_element_type=jnp.float32)
        southern = jnp.dot(legendre, flipped.T, preferred_element_type=jnp.float32)[::-1]
        return jnp.concatenate([northern, southern], axis=0).astype(jnp.bfloat16)
    fourier = lax.map(meridional, (spectra, live_mask, signed, basis))
    per_level = fourier.reshape(M, LAT, LEVELS, 2, 2).transpose(2, 0, 1, 3, 4)
    wave_f = zonal_tables(assign).astype(jnp.float32)
    inv_root = 1.0 / math.sqrt(LON)

    def zonal_section(level_block):
        grid_fields = jnp.einsum('kjfc,ckq->fjq', level_block.astype(jnp.float32), wave_f)
        scaled = grid_fields[0]
        upper_row = -jnp.roll(scaled[0], LON // 2, axis=-1)
        lower_row = -jnp.roll(scaled[-1], LON // 2, axis=-1)
        extended = jnp.concatenate([upper_row[None], scaled, lower_row[None]], axis=0)
        merid_v = grid_fields[1]
        vorticity = 0.5 * (jnp.roll(merid_v, -1, axis=-1) - jnp.roll(merid_v, 1, axis=-1)) - 0.5 * (extended[:-2] - extended[2:])
        flux = (vorticity * scaled).astype(jnp.bfloat16)
        zonal_back = jnp.einsum('jq,ckq->kjc', flux.astype(jnp.float32), wave_f) * inv_root
        return zonal_back.astype(jnp.bfloat16)
    zonal = lax.map(zonal_section, per_level)
    zonal = zonal.transpose(1, 2, 0, 3).reshape(M, LAT, LEVELS * 2)

    def project(inputs):
        returned, live_row, signed_row, legendre = inputs
        northern = jnp.dot(legendre.T, returned[:half_rows], preferred_element_type=jnp.float32)
        southern = jnp.dot(legendre.T, returned[half_rows:][::-1], preferred_element_type=jnp.float32)
        combined = live_row.astype(jnp.float32)[:, None] * northern + signed_row.astype(jnp.float32)[:, None] * southern
        return combined.reshape(M, LEVELS, 2).transpose(1, 2, 0)
    return lax.map(project, (zonal, live_mask, signed, basis))
```

```python
import functools
import math

import jax
import jax.numpy as jnp
from jax import lax
from jax.experimental import pallas as pl
from jax.experimental.pallas import tpu as pltpu
from jax.sharding import PartitionSpec as P

CHUNKS = 2


def zonal_tables(wavenums, lon):
    columns = jnp.arange(lon, dtype=jnp.int32)
    phases = wavenums[:, None] * columns[None, :] % lon
    angles = phases.astype(jnp.float32) * (2.0 * math.pi / lon)
    table = jnp.concatenate([jnp.cos(angles), jnp.sin(angles)], axis=0)
    return table.astype(jnp.bfloat16)


def zonal_kernel(scale, block, fields_ref, table_ref, out_ref, lines_ref, total_ref):
    my_rows, waves, lanes = fields_ref.shape
    span = lanes // 4

    @pl.when(pl.program_id(0) == 0)
    def _():
        total_ref[...] = jnp.zeros_like(total_ref)
        for j in range(my_rows):
            turned = fields_ref[j].astype(jnp.float32).T.astype(jnp.bfloat16)
            for g in range(2):
                for c in range(2):
                    part = turned[(2 * g + c) * span : (2 * g + c + 1) * span]
                    lines_ref[g, pl.ds(j * span, span), pl.ds(c * waves, waves)] = part

    @pl.loop(0, total_ref.shape[0] // block)
    def _(i):
        rows = pl.ds(pl.multiple_of(i * block, block), block)
        table = table_ref[...]
        wind = jnp.dot(lines_ref[0, rows, :], table, preferred_element_type=jnp.float32)
        vort = jnp.dot(lines_ref[1, rows, :], table, preferred_element_type=jnp.float32)
        flux = (wind * vort).astype(jnp.bfloat16)
        total_ref[rows, :] += lax.dot_general(
            flux, table, (((1,), (1,)), ((), ())), preferred_element_type=jnp.float32
        )

    @pl.when(pl.program_id(0) == pl.num_programs(0) - 1)
    def _():
        for j in range(my_rows):
            rows = total_ref[pl.ds(j * span, span), :] * scale
            both = jnp.concatenate([rows[:, :waves], rows[:, waves:]], axis=0)
            out_ref[j] = both.T.astype(jnp.bfloat16)


def zonal(fields, table):
    my_rows, waves, lanes = fields.shape
    span = lanes // 4
    lines = my_rows * span
    depth, lon = table.shape
    tile = math.gcd(lon, 256)
    block = math.gcd(lines, 320)
    return pl.pallas_call(
        functools.partial(zonal_kernel, 1.0 / math.sqrt(lon), block),
        grid=(lon // tile,),
        in_specs=[
            pl.BlockSpec((my_rows, waves, lanes), lambda i: (0, 0, 0)),
            pl.BlockSpec((depth, tile), lambda i: (0, i)),
        ],
        out_specs=pl.BlockSpec((my_rows, waves, 2 * span), lambda i: (0, 0, 0)),
        out_shape=jax.ShapeDtypeStruct((my_rows, waves, 2 * span), jnp.bfloat16),
        scratch_shapes=[
            pltpu.VMEM((2, lines, depth), jnp.bfloat16),
            pltpu.VMEM((lines, depth), jnp.float32),
        ],
        compiler_params=pltpu.CompilerParams(vmem_limit_bytes=40 * 1024 * 1024),
        cost_estimate=pl.CostEstimate(
            flops=6 * lines * depth * lon,
            bytes_accessed=6 * lines * depth + 2 * depth * lon,
            transcendentals=0,
        ),
    )(fields, table)


def body(assign, u_spec, v_spec, basis):
    slots, lev_dev, _, degrees = u_spec.shape
    rows = basis.shape[1]
    waves = assign.shape[0]
    lat_count = lax.axis_size("lat")
    lev_count = lax.axis_size("lev")
    lon = 4 * rows * lev_count
    lat_index = lax.axis_index("lat")
    lev_index = lax.axis_index("lev")
    step = lev_dev // CHUNKS
    levels = step * lev_count
    row_groups = math.gcd(lat_count, rows)
    lev_groups = lat_count // row_groups
    my_rows = rows // row_groups
    my_levels = levels // lev_groups

    my_waves = lax.dynamic_slice_in_dim(assign, lat_index * slots, slots)
    degree = jnp.arange(degrees, dtype=jnp.int32)
    live_mask = (degree[None, :] >= my_waves[:, None]).astype(jnp.int32)
    signed = live_mask * (1 - 2 * ((degree[None, :] + my_waves[:, None]) % 2))
    masks = jnp.stack([live_mask, signed], axis=1)
    masks_half = masks.astype(jnp.bfloat16)
    masks_full = masks.astype(jnp.float32)
    wave_sign = (1 - 2 * (my_waves % 2)).astype(jnp.float32)[:, None, None]
    parity = (1 - 2 * ((degree[None, :] + my_waves[:, None]) % 2)).astype(jnp.float32)
    parity = parity[:, None, :]
    slope = jnp.sin(my_waves.astype(jnp.float32) * (2.0 * math.pi / lon))
    slope = slope[:, None, None, None, None]

    forward = [(i, i + 1) for i in range(lev_count - 1)]
    backward = [(t, s) for s, t in forward]
    low = lax.ppermute(basis[:, -1:], "lev", forward).astype(jnp.float32)
    high = lax.ppermute(basis[:, :1], "lev", backward).astype(jnp.float32)
    wide = basis.astype(jnp.float32)
    low = jnp.where(lev_index == 0, -wave_sign * wide[:, :1], low)
    high = jnp.where(lev_index == lev_count - 1, parity * wide[:, -1:], high)
    above = jnp.concatenate([low, wide[:, :-1]], axis=1)
    below = jnp.concatenate([wide[:, 1:], high], axis=1)
    slant = (above - below).astype(jnp.bfloat16)
    table = zonal_tables(assign, lon)

    gathered = []
    for i in range(CHUNKS):
        both = [x[:, i * step : (i + 1) * step] for x in (u_spec, v_spec)]
        part = jnp.stack(both, axis=1).transpose(0, 1, 3, 2, 4)
        part = part.reshape(slots, 4 * step, degrees)
        gathered.append(lax.all_gather(part, "lev", axis=0))

    side = jnp.array([-0.5, 0.5], jnp.bfloat16)[:, None, None]
    arrived = []
    for i in range(CHUNKS):
        part = gathered[i].reshape(lev_count, slots, 2, 2, step, degrees)
        part = part.transpose(1, 2, 3, 0, 4, 5).reshape(slots, 2, 2, 1, levels, degrees)
        part = part * masks_half[:, None, None, :, None, :]
        wind = part[:, 0]
        other = part[:, 1].astype(jnp.float32) * slope
        merid = jnp.stack([other[:, 1], -other[:, 0]], axis=1).astype(jnp.bfloat16)
        tilt = wind * side
        head = jnp.stack([wind, merid], axis=1).reshape(slots, 8 * levels, degrees)
        tail = tilt.reshape(slots, 4 * levels, degrees)
        straight = jnp.einsum("kjn,krn->kjr", basis, head, preferred_element_type=jnp.float32)
        turned = jnp.einsum("kjn,krn->kjr", slant, tail, preferred_element_type=jnp.float32)
        send = straight + jnp.pad(turned, ((0, 0), (0, 0), (4 * levels, 0)))
        send = send.astype(jnp.bfloat16).transpose(1, 0, 2)
        if lev_groups > 1:
            send = send.reshape(row_groups, my_rows, slots, 8, lev_groups, my_levels)
            send = send.transpose(0, 4, 1, 2, 3, 5)
        send = send.reshape(lat_count, my_rows, slots, 8 * my_levels)
        arrived.append(lax.all_to_all(send, "lat", split_axis=0, concat_axis=0, tiled=True))

    backs = []
    for i in range(CHUNKS):
        block = arrived[i].transpose(1, 0, 2, 3).reshape(my_rows, waves, 8 * my_levels)
        backs.append(zonal(block, table))
    back = jnp.concatenate(backs, axis=2).reshape(my_rows, lat_count, slots, -1)
    back = back.transpose(1, 0, 2, 3)
    block = lax.all_to_all(back, "lat", split_axis=0, concat_axis=0, tiled=True)
    if lev_groups > 1:
        block = block.reshape(row_groups, lev_groups, my_rows, slots, 4 * CHUNKS, my_levels)
        block = block.transpose(0, 2, 3, 4, 1, 5)
    block = block.reshape(rows, slots, CHUNKS * 4 * levels).transpose(1, 0, 2)

    results = []
    for i in range(CHUNKS):
        part = block[:, :, i * 4 * levels : (i + 1) * 4 * levels]
        product = jnp.einsum("kjr,kjn->krn", part, basis, preferred_element_type=jnp.float32)
        product = product.reshape(slots, 2, 2, levels, degrees)
        total = (
            product[:, :, 0] * masks_full[:, None, :1, :]
            + product[:, :, 1] * masks_full[:, None, 1:, :]
        )
        total = total.astype(jnp.bfloat16).reshape(slots, 2, lev_count, step, degrees)
        total = total.transpose(2, 1, 3, 0, 4).reshape(lev_count * 2 * step, slots * degrees)
        total = lax.psum_scatter(total, "lev", scatter_dimension=0, tiled=True)
        results.append(total.reshape(2, step, slots, degrees))
    result = jnp.concatenate(results, axis=1).transpose(2, 1, 0, 3)
    return result.astype(jnp.float32)


def solution(mesh):
    return jax.shard_map(
        body,
        mesh=mesh,
        in_specs=(
            P(),
            P("lat", "lev", None, None),
            P("lat", "lev", None, None),
            P("lat", "lev", None),
        ),
        out_specs=P("lat", "lev", None, None),
        check_vma=False,
    )
```
